32 devices in a mesh: gx: 4 (over y, core), gy: 2 (over x), gz: 4 (over z).
Axes of the slice: x: 2, y: 2, z: 4, core: 2. Of those that a mesh axis runs over, the one named last changes fastest.
Arguments:
- positions: float32 [3, 4, 2, 4, 512], P(None, 'gx', 'gy', 'gz'), may hold values from 0 to 1
- velocities: float32 [3, 4, 2, 4, 512], P(None, 'gx', 'gy', 'gz'), may hold values from -6 to 6
- charges: float32 [4, 2, 4, 512], P('gx', 'gy', 'gz'), may hold values from -5 to 5
- cluster_atoms: int32 [4, 2, 4, 768], P('gx', 'gy', 'gz'), may hold values from 0 to 512, as said below
- pair_list: int32 [3, 4, 2, 4, 256], P(None, 'gx', 'gy', 'gz'), may hold values from 0 to 124, as said below
Outputs:
- new_positions: float32 [3, 4, 2, 4, 512], P(None, 'gx', 'gy', 'gz')
- new_velocities: float32 [3, 4, 2, 4, 512], P(None, 'gx', 'gy', 'gz')
- last_forces: float32 [3, 4, 2, 4, 512], P(None, 'gx', 'gy', 'gz')
The draws below stay inside these ranges and needn't reach their ends.
Inputs may be any that keep to these rules, and one draw needn't show every extreme that they name: `cluster_atoms`: on every domain each atom index below 512 stands in exactly one slot; all other slots hold 512, meaning empty. `pair_list`: row 0 and row 1 lie in 0 to 5, row 2 in 0 to 124; on every domain each of the 125 shift indices appears in at least 2 listed pairs.
All inputs are finite; a program needn't handle non-finite values.
Results may differ from the reference program's by a relative error of at most 0.0001.
Values sent between devices are 32-bit elements; how exact they have to be, the bound alone decides.
A program may use at most 64 MiB of HBM per device.

```python
import jax
import jax.numpy as jnp
from jax import lax

CLUSTER = 128
A_DEV = 512
CL_DEV = 6
PAIRS_DEV = 256
STEPS = 2
N_GX = 4
N_GY = 2
N_GZ = 4


def draw_cluster_atoms(key, part):
    device_count = N_GX * N_GY * N_GZ
    slot_count = CL_DEV * CLUSTER

    def per_device(device_key):
        shuffled = jax.random.permutation(device_key, jnp.arange(slot_count, dtype=jnp.int32))
        return jnp.minimum(shuffled, A_DEV).astype(jnp.int32)
    tables = jax.vmap(per_device)(jax.random.split(jax.random.fold_in(key, 11), device_count))
    return tables.reshape(N_GX, N_GY, N_GZ, slot_count)


def draw_pair_list(key, part):
    device_count = N_GX * N_GY * N_GZ
    pair_count = PAIRS_DEV
    covered = 125 * (pair_count // 125)

    def per_device(device_key):
        sub_keys = jax.random.split(device_key, 4)
        ordinal = jnp.arange(pair_count, dtype=jnp.int32)
        extra_shift = jax.random.randint(sub_keys[0], (pair_count,), 0, 125, dtype=jnp.int32)
        shift_index = jnp.where(ordinal < covered, ordinal % 125, extra_shift)
        shift_index = jax.random.permutation(sub_keys[1], shift_index)
        left_cluster = jax.random.randint(sub_keys[2], (pair_count,), 0, CL_DEV, dtype=jnp.int32)
        right_cluster = jax.random.randint(sub_keys[3], (pair_count,), 0, CL_DEV, dtype=jnp.int32)
        return jnp.stack([left_cluster, right_cluster, shift_index])
    pair_rows = jax.vmap(per_device)(jax.random.split(jax.random.fold_in(key, 23), device_count))
    return jnp.transpose(pair_rows, (1, 0, 2)).reshape(3, N_GX, N_GY, N_GZ, pair_count).astype(jnp.int32)


def block_levels(own_key, shape, cuts, smallest, largest):
    factor_of = 1.0
    for position, blocks in cuts:
        steps = jax.random.uniform(jax.random.fold_in(jax.random.fold_in(own_key, 6), position), (blocks,), jnp.float32, smallest / len(cuts), largest / len(cuts))
        factor_of = factor_of * jnp.repeat(jnp.exp(steps), shape[position] // blocks).reshape((-1,) + (1,) * (len(shape) - 1 - position))
    return factor_of


def noise(key, shape, spread, bound, pieces=(), held_as=jnp.bfloat16):
    values = jax.random.normal(key, shape, jnp.float32) * spread
    if len(pieces) > 0:
        values = block_levels(key, shape, pieces, -0.22, 0.18) * values
    return jnp.clip(values, min=-bound, max=bound).astype(held_as)


def setup_inputs(seed: int = 0) -> dict:
    splits = jax.random.split(jax.random.key(seed), 6)
    positions = jnp.clip(1.0 * jax.random.uniform(splits[0], (3, N_GX, N_GY, N_GZ, A_DEV), jnp.float32) ** block_levels(splits[0], (3, N_GX, N_GY, N_GZ, A_DEV), ((1, 4), (2, 2), (3, 4)), -0.2, 0.2), 0.0, 1.0)
    velocities = noise(splits[1], (3, N_GX, N_GY, N_GZ, A_DEV), 1.0, 6.0, ((1, 4), (2, 2), (3, 4)), jnp.float32)
    charges = noise(splits[2], (N_GX, N_GY, N_GZ, A_DEV), 1.0, 5.0, ((0, 4), (1, 2), (2, 4)), jnp.float32)
    cluster_atoms = draw_cluster_atoms(jax.random.fold_in(splits[5], 71), 0)
    pair_list = draw_pair_list(jax.random.fold_in(splits[5], 71), 0)
    return {"positions": positions, "velocities": velocities, "charges": charges, "cluster_atoms": cluster_atoms, "pair_list": pair_list}


CUTOFF_SQ = 4.0
SOFTENING = 0.5
TIME_STEP = 0.02


def pair_terms(left_xyz, left_charge, right_xyz, right_charge):
    separation = left_xyz[:, :, :, None] - right_xyz[:, :, None, :]
    distance_sq = jnp.sum(separation * separation, axis=0)
    window_term = jnp.maximum(1.0 - distance_sq / CUTOFF_SQ, 0.0)
    inverse = 1.0 / (distance_sq + SOFTENING)
    scalar = 2.0 * left_charge[:, :, None] * right_charge[:, None, :] * (
        3.0 * window_term * window_term * inverse / CUTOFF_SQ
        + window_term * window_term * window_term * inverse * inverse)
    pair_force = scalar[None] * separation
    return jnp.sum(pair_force, axis=3), -jnp.sum(pair_force, axis=2)


def forces_of(coords, atom_slots, slot_charge, left_rows, right_rows, offsets):
    device_count = atom_slots.shape[0]
    slot_count = atom_slots.shape[1]
    padded = jnp.concatenate([coords, jnp.zeros((3, device_count, 1), jnp.float32)], axis=2)
    slot_xyz = jnp.take_along_axis(padded, jnp.broadcast_to(atom_slots[None], (3, device_count, slot_count)), axis=2)
    slot_xyz = slot_xyz.reshape(3, device_count * CL_DEV, CLUSTER)
    block_size = 64
    blocks = left_rows.shape[0] // block_size

    def accumulate(carried, block_data):
        rows_left, rows_right, shift_vec = block_data
        left_xyz = slot_xyz[:, rows_left]
        right_xyz = slot_xyz[:, rows_right] + shift_vec[:, :, None]
        left_force, right_force = pair_terms(left_xyz, slot_charge[rows_left], right_xyz, slot_charge[rows_right])
        carried = carried.at[:, rows_left].add(left_force).at[:, rows_right].add(right_force)
        return carried, None

    start = jnp.zeros((3, device_count * CL_DEV, CLUSTER), jnp.float32)
    summed, _ = lax.scan(accumulate, start, (left_rows.reshape(blocks, block_size), right_rows.reshape(blocks, block_size), jnp.transpose(offsets.reshape(3, blocks, block_size), (1, 0, 2))))
    summed = summed.reshape(3, device_count, slot_count)

    def to_atoms(slot_force, slot_index):
        return jnp.zeros((3, A_DEV + 1), jnp.float32).at[:, slot_index].add(slot_force)[:, :A_DEV]

    return jax.vmap(to_atoms, in_axes=(1, 0), out_axes=1)(summed, atom_slots)


def reference(positions, velocities, charges, cluster_atoms, pair_list):
    device_count = N_GX * N_GY * N_GZ
    slot_count = CL_DEV * CLUSTER
    atom_slots = cluster_atoms.reshape(device_count, slot_count).astype(jnp.int32)
    charge_pad = jnp.concatenate([charges.reshape(device_count, A_DEV), jnp.zeros((device_count, 1), jnp.float32)], axis=1)
    slot_charge = jnp.take_along_axis(charge_pad, atom_slots, axis=1).reshape(device_count * CL_DEV, CLUSTER)
    pairs = pair_list.reshape(3, device_count, PAIRS_DEV).astype(jnp.int32)
    device = jnp.arange(device_count, dtype=jnp.int32)[:, None]
    cell_x = device // (N_GY * N_GZ)
    cell_y = (device // N_GZ) % N_GY
    cell_z = device % N_GZ
    shift_index = pairs[2]
    delta_x = shift_index // 25 - 2
    delta_y = (shift_index // 5) % 5 - 2
    delta_z = shift_index % 5 - 2
    source = (((cell_x + delta_x) % N_GX) * N_GY + (cell_y + delta_y) % N_GY) * N_GZ + (cell_z + delta_z) % N_GZ
    left_rows = (device * CL_DEV + pairs[0]).reshape(-1).astype(jnp.int32)
    right_rows = (source * CL_DEV + pairs[1]).reshape(-1).astype(jnp.int32)
    offsets = jnp.stack([delta_x, delta_y, delta_z]).reshape(3, -1).astype(jnp.float32)
    coords = positions.reshape(3, device_count, A_DEV)
    velocity = velocities.reshape(3, device_count, A_DEV)
    forces = jnp.zeros_like(coords)
    for step_index in range(STEPS):
        forces = forces_of(coords, atom_slots, slot_charge, left_rows, right_rows, offsets)
        velocity = velocity + TIME_STEP * forces
        coords = coords + TIME_STEP * velocity
    return coords.reshape(positions.shape), velocity.reshape(positions.shape), forces.reshape(positions.shape)
```

```python
import functools

import jax
import jax.numpy as jnp
from jax import lax
from jax.experimental import pallas as pl
from jax.experimental.pallas import tpu as pltpu
from jax.sharding import PartitionSpec as P

CLUSTER = 128
STEPS = 2
TIME_STEP = 0.02
MESH = pl.DeviceIdType.MESH
AXES = ("gx", "gy", "gz")
VMEM = pl.BlockSpec(memory_space=pltpu.VMEM)
SMEM = pl.BlockSpec(memory_space=pltpu.SMEM)
UNROLL = 4


def split3(value):
    hi = value.astype(jnp.bfloat16)
    rest = value - hi.astype(jnp.float32)
    mid = rest.astype(jnp.bfloat16)
    lo = (rest - mid.astype(jnp.float32)).astype(jnp.bfloat16)
    return hi, mid, lo


class Zone:
    def __init__(self, sizes):
        self.sizes = sizes
        self.spans = tuple(min(5, n) for n in sizes)
        self.lows = tuple(-2 if n >= 5 else 0 for n in sizes)
        self.count = self.spans[0] * self.spans[1] * self.spans[2]
        own = tuple(-low for low in self.lows)
        self.own = (own[0] * self.spans[1] + own[1]) * self.spans[2] + own[2]

    def place(self, deltas):
        index = 0
        for delta, n, span in zip(deltas, self.sizes, self.spans):
            if n >= 5:
                here = delta + 2
            elif n in (1, 2, 4):
                here = (delta + 2 * n) & (n - 1)
            else:
                here = lax.rem(delta + 2 * n, n)
            index = index * span + here
        return index

    def peer(self, index, sign):
        parts = (
            index // (self.spans[1] * self.spans[2]),
            (index // self.spans[2]) % self.spans[1],
            index % self.spans[2],
        )
        out = []
        for axis, n, low, part in zip(AXES, self.sizes, self.lows, parts):
            out.append((lax.axis_index(axis) + sign * (part + low) + 2 * n) % n)
        return tuple(out)

    def others(self, body):
        def step(k, carry):
            body((self.own + 1 + k) % self.count)
            return carry

        lax.fori_loop(0, self.count - 1, step, 0)


def enter(zone):
    barrier = pltpu.get_barrier_semaphore()

    def greet(index):
        pl.semaphore_signal(barrier, 1, device_id=zone.peer(index, 1), device_id_type=MESH)

    zone.others(greet)
    pl.semaphore_wait(barrier, zone.count - 1)


def one_hot(atoms_ref, atom_count):
    slots = atoms_ref.shape[1]
    rows = lax.broadcasted_iota(jnp.int32, (atom_count, slots), 0)
    return jnp.where(rows == atoms_ref[...], 1.0, 0.0).astype(jnp.bfloat16)


def spread_kernel(zone, rows, x_ref, v_ref, q_ref, atoms_ref, zone_ref, vel_ref, send_sem, recv_sem):
    atom_count = x_ref.shape[1]
    clusters = atoms_ref.shape[1] // CLUSTER
    data = jnp.concatenate(
        [x_ref[...], v_ref[...], q_ref[...], jnp.zeros((1, atom_count), jnp.float32)], axis=0
    )
    hi, mid, lo = split3(data)
    stacked = jnp.concatenate([hi, mid, lo, jnp.zeros_like(hi)], axis=0)
    out = jnp.dot(stacked, one_hot(atoms_ref, atom_count), preferred_element_type=jnp.float32)
    slot = out[0:8] + out[8:16] + out[16:24]
    for k in range(clusters):
        lanes = slice(k * CLUSTER, (k + 1) * CLUSTER)
        for c in range(3):
            zone_ref[zone.own, c * clusters + k, :] = slot[c, lanes]
            vel_ref[c * clusters + k, :] = slot[3 + c, lanes]
        zone_ref[zone.own, 3 * clusters + k, :] = slot[6, lanes]
    enter(zone)
    share(zone, zone_ref, send_sem, recv_sem, 4 * clusters)


def share(zone, zone_ref, send_sem, recv_sem, rows):
    def copy(index):
        return pltpu.make_async_remote_copy(
            src_ref=zone_ref.at[zone.own, pl.ds(0, rows)],
            dst_ref=zone_ref.at[index, pl.ds(0, rows)],
            send_sem=send_sem.at[index],
            recv_sem=recv_sem.at[index],
            device_id=zone.peer(index, -1),
            device_id_type=MESH,
        )

    zone.others(lambda index: copy(index).start())
    zone.others(lambda index: copy(index).wait())


def gathered_force(zone, force_ref, land_ref, send_sem, recv_sem):
    def copy(index):
        return pltpu.make_async_remote_copy(
            src_ref=force_ref.at[index],
            dst_ref=land_ref.at[index],
            send_sem=send_sem.at[index],
            recv_sem=recv_sem.at[index],
            device_id=zone.peer(index, 1),
            device_id_type=MESH,
        )

    zone.others(lambda index: copy(index).start())
    zone.others(lambda index: copy(index).wait())

    def add(k, total):
        return total + land_ref[(zone.own + 1 + k) % zone.count]

    return lax.fori_loop(0, zone.count - 1, add, force_ref[zone.own])


def advance_kernel(
    zone, rows, force_ref, x_ref, vel_ref, zone_ref, new_vel_ref,
    land_ref, send_sem, recv_sem, send_sem2, recv_sem2,
):
    enter(zone)
    force = gathered_force(zone, force_ref, land_ref, send_sem, recv_sem)
    velocity = vel_ref[...] + TIME_STEP * force
    zone_ref[zone.own, pl.ds(0, rows)] = x_ref[...] + TIME_STEP * velocity
    new_vel_ref[...] = velocity
    share(zone, zone_ref, send_sem2, recv_sem2, rows)


def finish_kernel(
    zone, rows, force_ref, x_ref, vel_ref, atoms_ref, x_out, v_out, f_out,
    land_ref, slot_ref, send_sem, recv_sem,
):
    slots = atoms_ref.shape[1]
    clusters = slots // CLUSTER
    atom_count = x_out.shape[1]
    enter(zone)
    force = gathered_force(zone, force_ref, land_ref, send_sem, recv_sem)
    velocity = vel_ref[...] + TIME_STEP * force
    coords = x_ref[...] + TIME_STEP * velocity
    slot_ref[...] = jnp.zeros_like(slot_ref)
    for k in range(clusters):
        lanes = slice(k * CLUSTER, (k + 1) * CLUSTER)
        for c in range(3):
            r = c * clusters + k
            slot_ref[pl.ds(c, 1), lanes] = coords[r : r + 1]
            slot_ref[pl.ds(3 + c, 1), lanes] = velocity[r : r + 1]
            slot_ref[pl.ds(6 + c, 1), lanes] = force[r : r + 1]
    stacked = jnp.concatenate(split3(slot_ref[...]), axis=0)
    out = lax.dot_general(
        stacked, one_hot(atoms_ref, atom_count), (((1,), (1,)), ((), ())),
        preferred_element_type=jnp.float32,
    )
    atom = out[0:16] + out[16:32] + out[32:48]
    x_out[...] = atom[0:3]
    v_out[...] = atom[3:6]
    f_out[...] = atom[6:9]


def weighted(coords, charge):
    charge = 0.125 * charge
    part = jnp.concatenate([charge * c for c in coords] + [charge], axis=0)
    pieces = [p.astype(jnp.float32) for p in split3(part)]
    stacked = jnp.concatenate(pieces + [jnp.zeros_like(part)], axis=0).astype(jnp.bfloat16)
    return jnp.concatenate([stacked, stacked], axis=1)


def folded(out):
    return out[0:4] + out[4:8] + out[8:12]


def pair_kernel(zone, clusters, pairs_ref, x_ref, q_ref, force_ref, left_ref, lw_ref, acc_ref):
    own = zone.own
    for k in range(clusters):
        coords = []
        for c in range(3):
            row = x_ref[own, pl.ds(c * clusters + k, 1), :]
            coords.append(row)
            left_ref[k, c] = jnp.transpose(jnp.broadcast_to(0.5 * row, (CLUSTER, CLUSTER)))
        lw_ref[k] = weighted(coords, q_ref[own, pl.ds(3 * clusters + k, 1), :])
    acc_ref[...] = jnp.zeros_like(acc_ref)
    force_ref[...] = jnp.zeros_like(force_ref)

    def one(p):
        i = pairs_ref[0, p]
        j = pairs_ref[1, p]
        t = pairs_ref[2, p]
        t25 = (t * 5243) >> 17
        t5 = (t * 205) >> 10
        deltas = (t25 - 2, t5 - 5 * t25 - 2, t - 5 * t5 - 2)
        z = zone.place(deltas)
        coords = [
            x_ref[z, pl.ds(c * clusters + j, 1), :] + deltas[c].astype(jnp.float32)
            for c in range(3)
        ]
        charge = q_ref[z, pl.ds(3 * clusters + j, 1), :]
        r2 = None
        for c in range(3):
            d = left_ref[i, c] - 0.5 * coords[c]
            r2 = d * d if r2 is None else r2 + d * d
        g = jnp.maximum(1.0 - r2, 0.0)
        t = g * (1.0 / (r2 + 0.125))
        f = (g * t) * (t + 3.0)
        hi = f.astype(jnp.bfloat16)
        lo = (f - hi.astype(jnp.float32)).astype(jnp.bfloat16)
        out_left = lax.dot_general(
            weighted(coords, charge), jnp.concatenate([hi, lo], axis=1),
            (((1,), (1,)), ((), ())), preferred_element_type=jnp.float32,
        )
        out_right = jnp.dot(
            lw_ref[i], jnp.concatenate([hi, lo], axis=0), preferred_element_type=jnp.float32
        )
        return i, j, z, coords, charge, out_left, out_right

    def block(b, carry):
        done = [one(b * UNROLL + n) for n in range(UNROLL)]
        for i, j, z, coords, charge, out_left, out_right in done:
            acc_ref[i] += out_left
            sums = folded(out_right)
            for c in range(3):
                row = pl.ds(c * clusters + j, 1)
                force_ref[z, row, :] += charge * (coords[c] * sums[3:4] - sums[c : c + 1])
        return carry

    lax.fori_loop(0, pairs_ref.shape[1] // UNROLL, block, 0)
    for k in range(clusters):
        sums = folded(acc_ref[k])
        charge = q_ref[own, pl.ds(3 * clusters + k, 1), :]
        for c in range(3):
            row = pl.ds(c * clusters + k, 1)
            force_ref[own, row, :] += charge * (x_ref[own, row, :] * sums[3:4] - sums[c : c + 1])


def shards(sizes, positions, velocities, charges, cluster_atoms, pair_list):
    zone = Zone(sizes)
    atom_count = positions.shape[-1]
    slots = cluster_atoms.shape[-1]
    clusters = slots // CLUSTER
    rows = 3 * clusters
    f32 = jnp.float32
    x = positions.reshape(3, atom_count)
    v = velocities.reshape(3, atom_count)
    q = charges.reshape(1, atom_count)
    atoms = cluster_atoms.reshape(1, slots)
    pairs = pair_list.reshape(3, pair_list.shape[-1])
    sems = [pltpu.SemaphoreType.DMA((zone.count,))] * 2
    land = pltpu.VMEM((zone.count, rows, CLUSTER), f32)

    def params(number):
        return pltpu.CompilerParams(collective_id=number, has_side_effects=True)

    zone_shape = jax.ShapeDtypeStruct((zone.count, 4 * clusters, CLUSTER), f32)
    vel_shape = jax.ShapeDtypeStruct((rows, CLUSTER), f32)
    zone_x, vel = pl.pallas_call(
        functools.partial(spread_kernel, zone, rows),
        out_shape=(zone_shape, vel_shape),
        in_specs=[VMEM] * 4,
        out_specs=(VMEM, VMEM),
        scratch_shapes=sems,
        compiler_params=params(0),
        name="spread",
    )(x, v, q, atoms)
    zone_q = zone_x
    pair_call = pl.pallas_call(
        functools.partial(pair_kernel, zone, clusters),
        out_shape=jax.ShapeDtypeStruct((zone.count, rows, CLUSTER), f32),
        in_specs=[SMEM, VMEM, VMEM],
        out_specs=VMEM,
        scratch_shapes=[
            pltpu.VMEM((clusters, 3, CLUSTER, CLUSTER), f32),
            pltpu.VMEM((clusters, 16, 2 * CLUSTER), jnp.bfloat16),
            pltpu.VMEM((clusters, 16, CLUSTER), f32),
        ],
        name="pairs",
    )
    for step in range(STEPS):
        force = pair_call(pairs, zone_x, zone_q)
        own_x = zone_x[zone.own, :rows]
        if step < STEPS - 1:
            zone_x, vel = pl.pallas_call(
                functools.partial(advance_kernel, zone, rows),
                out_shape=(zone_shape, vel_shape),
                in_specs=[VMEM] * 3,
                out_specs=(VMEM, VMEM),
                scratch_shapes=[land] + sems + sems,
                compiler_params=params(1 + step),
                name="advance",
            )(force, own_x, vel)
        else:
            shape = jax.ShapeDtypeStruct((3, atom_count), f32)
            outs = pl.pallas_call(
                functools.partial(finish_kernel, zone, rows),
                out_shape=(shape, shape, shape),
                in_specs=[VMEM] * 4,
                out_specs=(VMEM, VMEM, VMEM),
                scratch_shapes=[land, pltpu.VMEM((16, slots), f32)] + sems,
                compiler_params=params(1 + step),
                name="finish",
            )(force, own_x, vel, atoms)
    return tuple(out.reshape(positions.shape) for out in outs)


def solution(mesh):
    spec3 = P(None, "gx", "gy", "gz", None)
    spec1 = P("gx", "gy", "gz", None)
    sizes = tuple(mesh.shape[axis] for axis in AXES)
    return jax.shard_map(
        functools.partial(shards, sizes),
        mesh=mesh,
        in_specs=(spec3, spec3, spec1, spec1, spec3),
        out_specs=(spec3, spec3, spec3),
        check_vma=False,
    )
```

```python
import functools

import jax
import jax.numpy as jnp
from jax import lax
from jax.experimental import pallas as pl
from jax.experimental.pallas import tpu as pltpu
from jax.sharding import PartitionSpec as P

CLUSTER = 128
STEPS = 2
TIME_STEP = 0.02
MESH = pl.DeviceIdType.MESH
AXES = ("gx", "gy", "gz")
VMEM = pl.BlockSpec(memory_space=pltpu.VMEM)
SMEM = pl.BlockSpec(memory_space=pltpu.SMEM)
UNROLL = 4


def split3(value):
    hi = value.astype(jnp.bfloat16)
    rest = value - hi.astype(jnp.float32)
    mid = rest.astype(jnp.bfloat16)
    lo = (rest - mid.astype(jnp.float32)).astype(jnp.bfloat16)
    return hi, mid, lo


class Zone:
    def __init__(self, sizes):
        self.sizes = sizes
        self.spans = tuple(min(5, n) for n in sizes)
        self.lows = tuple(-2 if n >= 5 else 0 for n in sizes)
        self.count = self.spans[0] * self.spans[1] * self.spans[2]
        own = tuple(-low for low in self.lows)
        self.own = (own[0] * self.spans[1] + own[1]) * self.spans[2] + own[2]

    def place(self, deltas):
        index = 0
        for delta, n, span in zip(deltas, self.sizes, self.spans):
            if n >= 5:
                here = delta + 2
            elif n in (1, 2, 4):
                here = (delta + 2 * n) & (n - 1)
            else:
                here = lax.rem(delta + 2 * n, n)
            index = index * span + here
        return index

    def peer(self, index, sign):
        parts = (
            index // (self.spans[1] * self.spans[2]),
            (index // self.spans[2]) % self.spans[1],
            index % self.spans[2],
        )
        out = []
        for axis, n, low, part in zip(AXES, self.sizes, self.lows, parts):
            out.append((lax.axis_index(axis) + sign * (part + low) + 2 * n) % n)
        return tuple(out)

    def others(self, body):
        def step(k, carry):
            body((self.own + 1 + k) % self.count)
            return carry

        lax.fori_loop(0, self.count - 1, step, 0)


def one_hot(atoms_ref, atom_count):
    slots = atoms_ref.shape[1]
    rows = lax.broadcasted_iota(jnp.int32, (atom_count, slots), 0)
    return jnp.where(rows == atoms_ref[...], 1.0, 0.0).astype(jnp.bfloat16)


def rows_where(count, index):
    rows = lax.broadcasted_iota(jnp.int32, (count, index.shape[1]), 0)
    return jnp.where(rows == index, 1.0, 0.0).astype(jnp.bfloat16)


def exact_dot(selector, values):
    return sum(
        jnp.dot(selector, piece, preferred_element_type=jnp.float32) for piece in split3(values)
    )


def side_by_side(ref):
    return jnp.concatenate([ref[c] for c in range(ref.shape[0])], axis=1)


def share(zone, src, dst_ref, send_sem, recv_sem):
    def copy(index):
        return pltpu.make_async_remote_copy(
            src_ref=src,
            dst_ref=dst_ref.at[index],
            send_sem=send_sem.at[index],
            recv_sem=recv_sem.at[index],
            device_id=zone.peer(index, -1),
            device_id_type=MESH,
        )

    zone.others(lambda index: copy(index).start())
    zone.others(lambda index: copy(index).wait())


def gathered_force(zone, force_ref, land_ref, send_sem, recv_sem):
    def copy(index):
        return pltpu.make_async_remote_copy(
            src_ref=force_ref.at[index],
            dst_ref=land_ref.at[index],
            send_sem=send_sem.at[index],
            recv_sem=recv_sem.at[index],
            device_id=zone.peer(index, 1),
            device_id_type=MESH,
        )

    zone.others(lambda index: copy(index).start())
    zone.others(lambda index: copy(index).wait())

    def add(k, total):
        return total + land_ref[(zone.own + 1 + k) % zone.count]

    return lax.fori_loop(0, zone.count - 1, add, force_ref[zone.own])


def weighted(coords, charge):
    charge = 0.125 * charge
    part = jnp.concatenate([charge * c for c in coords] + [charge], axis=0)
    pieces = [p.astype(jnp.float32) for p in split3(part)]
    stacked = jnp.concatenate(pieces + [jnp.zeros_like(part)], axis=0).astype(jnp.bfloat16)
    return jnp.concatenate([stacked, stacked], axis=1)


def folded(out):
    return out[0:4] + out[4:8] + out[8:12]


def shift_of(t):
    t25 = (t * 5243) >> 17
    t5 = (t * 205) >> 10
    return t25 - 2, t5 - 5 * t25 - 2, t - 5 * t5 - 2


def pair_forces(zone, clusters, pairs_ref, x_ref, q_ref, force_ref, left_ref, lw_ref,
                f_ref, right_sum_ref, left_sum_ref, zone_hot_ref, home_hot_ref):
    own = zone.own
    for k in range(clusters):
        coords = []
        for c in range(3):
            row = x_ref[own, pl.ds(c * clusters + k, 1), :]
            coords.append(row)
            left_ref[k, c] = jnp.transpose(jnp.broadcast_to(0.5 * row, (CLUSTER, CLUSTER)))
        lw_ref[k] = weighted(coords, q_ref[own, pl.ds(3 * clusters + k, 1), :])

    def right_side(p):
        j = pairs_ref[1, 0, p]
        deltas = shift_of(pairs_ref[2, 0, p])
        z = zone.place(deltas)
        coords = [
            x_ref[z, pl.ds(c * clusters + j, 1), :] + deltas[c].astype(jnp.float32)
            for c in range(3)
        ]
        return coords, q_ref[z, pl.ds(3 * clusters + j, 1), :]

    def geometry(b):
        for n in range(UNROLL):
            p = b * UNROLL + n
            coords, _ = right_side(p)
            i = pairs_ref[0, 0, p]
            r2 = None
            for c in range(3):
                d = left_ref[i, c] - 0.5 * coords[c]
                r2 = d * d if r2 is None else r2 + d * d
            g = jnp.maximum(1.0 - r2, 0.0)
            den = r2 + 0.125
            start = pl.reciprocal(den, approx=True)
            t = (g * start) * (2.0 - den * start)
            f = (g * t) * (t + 3.0)
            hi = f.astype(jnp.bfloat16)
            f_ref[n, 0] = hi
            f_ref[n, 1] = (f - hi.astype(jnp.float32)).astype(jnp.bfloat16)

    def sums(b):
        found = []
        for n in range(UNROLL):
            p = b * UNROLL + n
            hi, lo = f_ref[n, 0], f_ref[n, 1]
            coords, charge = right_side(p)
            left = lax.dot_general(
                weighted(coords, charge), jnp.concatenate([hi, lo], axis=1),
                (((1,), (1,)), ((), ())), preferred_element_type=jnp.float32,
            )
            right = jnp.dot(
                lw_ref[pairs_ref[0, 0, p]], jnp.concatenate([hi, lo], axis=0),
                preferred_element_type=jnp.float32,
            )
            found.append((p, coords, charge, left, right))
        return found

    def keep(found):
        for p, coords, charge, left, right in found:
            left = folded(left)
            right = folded(right)
            for c in range(4):
                left_sum_ref[c, pl.ds(p, 1), :] = left[c : c + 1]
            for c in range(3):
                right_sum_ref[c, pl.ds(p, 1), :] = charge * (
                    coords[c] * right[3:4] - right[c : c + 1]
                )

    blocks = pairs_ref.shape[2] // UNROLL
    geometry(0)

    def block(b, carry):
        found = sums(b - 1)
        geometry(b)
        keep(found)
        return carry

    lax.fori_loop(1, blocks, block, 0)
    keep(sums(blocks - 1))

    zone_out = exact_dot(zone_hot_ref[...], side_by_side(right_sum_ref))
    home_out = exact_dot(home_hot_ref[...], side_by_side(left_sum_ref))
    for z in range(zone.count):
        for c in range(3):
            force_ref[z, c * clusters : (c + 1) * clusters, :] = zone_out[
                z * 8 : z * 8 + clusters, c * CLUSTER : (c + 1) * CLUSTER
            ]
    for c in range(3):
        rows = slice(c * clusters, (c + 1) * clusters)
        total = home_out[0:clusters, 3 * CLUSTER :]
        moment = home_out[0:clusters, c * CLUSTER : (c + 1) * CLUSTER]
        charge = q_ref[own, 3 * clusters : 4 * clusters, :]
        force_ref[own, rows, :] += charge * (x_ref[own, rows, :] * total - moment)


def kernel(zone, pairs_ref, pairs_vec_ref, x_in, v_in, q_in, atoms_ref, x_out, v_out, f_out,
           zone0_ref, zone1_ref, vel_ref, pos_ref, force_ref, land_ref, slot_ref, left_ref, lw_ref, f_ref,
           right_sum_ref, left_sum_ref, zone_hot_ref, home_hot_ref, send_sem, recv_sem):
    atom_count = x_in.shape[2]
    slots = atoms_ref.shape[1]
    clusters = slots // CLUSTER
    rows = 3 * clusters
    own = zone.own
    barrier = pltpu.get_barrier_semaphore()
    zone.others(lambda index: pl.semaphore_signal(
        barrier, 1, device_id=zone.peer(index, 1), device_id_type=MESH))

    data = jnp.concatenate(
        [x_in[c] for c in range(3)] + [v_in[c] for c in range(3)]
        + [q_in[...], jnp.zeros((1, atom_count), jnp.float32)], axis=0
    )
    hi, mid, lo = split3(data)
    stacked = jnp.concatenate([hi, mid, lo, jnp.zeros_like(hi)], axis=0)
    out = jnp.dot(stacked, one_hot(atoms_ref, atom_count), preferred_element_type=jnp.float32)
    slot = out[0:8] + out[8:16] + out[16:24]
    for k in range(clusters):
        lanes = slice(k * CLUSTER, (k + 1) * CLUSTER)
        for c in range(3):
            zone0_ref[own, c * clusters + k, :] = slot[c, lanes]
            vel_ref[c * clusters + k, :] = slot[3 + c, lanes]
        zone0_ref[own, 3 * clusters + k, :] = slot[6, lanes]
    deltas = shift_of(pairs_vec_ref[2])
    zone_hot_ref[...] = rows_where(zone.count * 8, zone.place(deltas) * 8 + pairs_vec_ref[1])
    home_hot_ref[...] = rows_where(8, pairs_vec_ref[0])
    pl.semaphore_wait(barrier, zone.count - 1)
    share(zone, zone0_ref.at[own], zone0_ref, send_sem.at[0], recv_sem.at[0])

    for step in range(STEPS):
        x_ref = zone0_ref if step == 0 else zone1_ref.at[step - 1]
        pair_forces(zone, clusters, pairs_ref, x_ref, zone0_ref, force_ref, left_ref, lw_ref,
                    f_ref, right_sum_ref, left_sum_ref, zone_hot_ref, home_hot_ref)
        force = gathered_force(zone, force_ref, land_ref.at[step],
                               send_sem.at[2 * step + 1], recv_sem.at[2 * step + 1])
        velocity = vel_ref[...] + TIME_STEP * force
        coords = x_ref[own, 0:rows, :] + TIME_STEP * velocity
        if step < STEPS - 1:
            vel_ref[...] = velocity
            zone1_ref[step, own] = coords
            share(zone, zone1_ref.at[step, own], zone1_ref.at[step],
                  send_sem.at[2 * step + 2], recv_sem.at[2 * step + 2])

    slot_ref[...] = jnp.zeros_like(slot_ref)
    for k in range(clusters):
        lanes = slice(k * CLUSTER, (k + 1) * CLUSTER)
        for c in range(3):
            r = c * clusters + k
            slot_ref[pl.ds(c, 1), lanes] = coords[r : r + 1]
            slot_ref[pl.ds(3 + c, 1), lanes] = velocity[r : r + 1]
            slot_ref[pl.ds(6 + c, 1), lanes] = force[r : r + 1]
    stacked = jnp.concatenate(split3(slot_ref[...]), axis=0)
    out = lax.dot_general(
        stacked, one_hot(atoms_ref, atom_count), (((1,), (1,)), ((), ())),
        preferred_element_type=jnp.float32,
    )
    atom = out[0:16] + out[16:32] + out[32:48]
    for c in range(3):
        x_out[c] = atom[c : c + 1]
        v_out[c] = atom[3 + c : 4 + c]
        f_out[c] = atom[6 + c : 7 + c]


def shards(sizes, positions, velocities, charges, cluster_atoms, pair_list):
    zone = Zone(sizes)
    atom_count = positions.shape[-1]
    slots = cluster_atoms.shape[-1]
    pair_count = pair_list.shape[-1]
    clusters = slots // CLUSTER
    rows = 3 * clusters
    f32, bf16 = jnp.float32, jnp.bfloat16
    x = positions.reshape(3, 1, atom_count)
    v = velocities.reshape(3, 1, atom_count)
    q = charges.reshape(1, atom_count)
    atoms = cluster_atoms.reshape(1, slots)
    pairs = pair_list.reshape(3, 1, pair_count)
    shape = jax.ShapeDtypeStruct((3, 1, atom_count), f32)
    outs = pl.pallas_call(
        functools.partial(kernel, zone),
        out_shape=(shape, shape, shape),
        in_specs=[SMEM] + [VMEM] * 5,
        out_specs=(VMEM, VMEM, VMEM),
        scratch_shapes=[
            pltpu.VMEM((zone.count, 4 * clusters, CLUSTER), f32),
            pltpu.VMEM((STEPS - 1, zone.count, rows, CLUSTER), f32),
            pltpu.VMEM((rows, CLUSTER), f32),
            pltpu.VMEM((rows, CLUSTER), f32),
            pltpu.VMEM((zone.count, rows, CLUSTER), f32),
            pltpu.VMEM((STEPS, zone.count, rows, CLUSTER), f32),
            pltpu.VMEM((16, slots), f32),
            pltpu.VMEM((clusters, 3, CLUSTER, CLUSTER), f32),
            pltpu.VMEM((clusters, 16, 2 * CLUSTER), bf16),
            pltpu.VMEM((UNROLL, 2, CLUSTER, CLUSTER), bf16),
            pltpu.VMEM((3, pair_count, CLUSTER), f32),
            pltpu.VMEM((4, pair_count, CLUSTER), f32),
            pltpu.VMEM((zone.count * 8, pair_count), bf16),
            pltpu.VMEM((8, pair_count), bf16),
            pltpu.SemaphoreType.DMA((2 * STEPS, zone.count)),
            pltpu.SemaphoreType.DMA((2 * STEPS, zone.count)),
        ],
        compiler_params=pltpu.CompilerParams(collective_id=0, has_side_effects=True),
        name="leapfrog",
    )(pairs, pairs, x, v, q, atoms)
    return tuple(out.reshape(positions.shape) for out in outs)


def solution(mesh):
    spec3 = P(None, "gx", "gy", "gz", None)
    spec1 = P("gx", "gy", "gz", None)
    sizes = tuple(mesh.shape[axis] for axis in AXES)
    return jax.shard_map(
        functools.partial(shards, sizes),
        mesh=mesh,
        in_specs=(spec3, spec3, spec1, spec1, spec3),
        out_specs=(spec3, spec3, spec3),
        check_vma=False,
    )
```

```python
import functools

import jax
import jax.numpy as jnp
from jax import lax
from jax.experimental import pallas as pl
from jax.experimental.pallas import tpu as pltpu
from jax.sharding import PartitionSpec as P

CLUSTER = 128
STEPS = 2
TIME_STEP = 0.02
MESH = pl.DeviceIdType.MESH
AXES = ("gx", "gy", "gz")
VMEM = pl.BlockSpec(memory_space=pltpu.VMEM)
SMEM = pl.BlockSpec(memory_space=pltpu.SMEM)
UNROLL = 16


def split3(value):
    hi = value.astype(jnp.bfloat16)
    rest = value - hi.astype(jnp.float32)
    mid = rest.astype(jnp.bfloat16)
    lo = (rest - mid.astype(jnp.float32)).astype(jnp.bfloat16)
    return hi, mid, lo


class Zone:
    def __init__(self, sizes):
        self.sizes = sizes
        self.spans = tuple(min(5, n) for n in sizes)
        self.lows = tuple(-2 if n >= 5 else 0 for n in sizes)
        self.count = self.spans[0] * self.spans[1] * self.spans[2]
        own = tuple(-low for low in self.lows)
        self.paired = max(sizes) <= 4 and sizes[0] % 2 == 0
        self.plane = self.spans[1] * self.spans[2]
        self.own = (own[0] * self.spans[1] + own[1]) * self.spans[2] + own[2]

    def place(self, deltas):
        index = 0
        for delta, n, span in zip(deltas, self.sizes, self.spans):
            if n >= 5:
                here = delta + 2
            elif n in (1, 2, 4):
                here = (delta + 2 * n) & (n - 1)
            else:
                here = lax.rem(delta + 2 * n, n)
            index = index * span + here
        return index

    def peer(self, index, sign):
        parts = (
            index // (self.spans[1] * self.spans[2]),
            (index // self.spans[2]) % self.spans[1],
            index % self.spans[2],
        )
        out = []
        for axis, n, low, part in zip(AXES, self.sizes, self.lows, parts):
            out.append((lax.axis_index(axis) + sign * (part + low) + 2 * n) % n)
        return tuple(out)

    def turn(self):
        return 1 - 2 * (lax.axis_index(AXES[0]) % 2)

    def partner(self):
        return (lax.axis_index(AXES[0]) + self.turn(),) + tuple(
            lax.axis_index(axis) for axis in AXES[1:]
        )

    def seen_by_partner(self, index):
        return (index - self.turn() * self.plane + self.count) % self.count

    def alike(self, body):
        def step(k, carry):
            body((k // self.plane) * 2 * self.plane + k % self.plane)
            return carry

        lax.fori_loop(1, self.count // 2, step, 0)

    def others(self, body):
        def step(k, carry):
            body((self.own + 1 + k) % self.count)
            return carry

        lax.fori_loop(0, self.count - 1, step, 0)


def one_hot(atoms_ref, atom_count):
    slots = atoms_ref.shape[1]
    rows = lax.broadcasted_iota(jnp.int32, (atom_count, slots), 0)
    return jnp.where(rows == atoms_ref[...], 1.0, 0.0).astype(jnp.bfloat16)


def rows_where(count, index):
    rows = lax.broadcasted_iota(jnp.int32, (count, index.shape[1]), 0)
    return jnp.where(rows == index, 1.0, 0.0).astype(jnp.bfloat16)


def exact_dot(selector, values):
    return sum(
        jnp.dot(selector, piece, preferred_element_type=jnp.float32) for piece in split3(values)
    )


def side_by_side(ref):
    return jnp.concatenate([ref[c] for c in range(ref.shape[0])], axis=1)


def share(zone, src, dst_ref, send_sem, recv_sem):
    def copy(index):
        return pltpu.make_async_remote_copy(
            src_ref=src,
            dst_ref=dst_ref.at[index],
            send_sem=send_sem.at[index],
            recv_sem=recv_sem.at[index],
            device_id=zone.peer(index, -1),
            device_id_type=MESH,
        )

    if not zone.paired:
        zone.others(lambda index: copy(index).start())
        zone.others(lambda index: copy(index).wait())
        return

    def relay(index, block):
        place = zone.seen_by_partner(index)
        return pltpu.make_async_remote_copy(
            src_ref=block,
            dst_ref=dst_ref.at[place],
            send_sem=send_sem.at[(index + zone.plane) % zone.count],
            recv_sem=recv_sem.at[place],
            device_id=zone.partner(),
            device_id_type=MESH,
        )

    zone.alike(lambda index: copy(index).start())
    relay(zone.own, src).start()

    def pass_on(index):
        copy(index).wait_recv()
        relay(index, dst_ref.at[index]).start()

    zone.alike(pass_on)
    zone.alike(lambda index: copy(index).wait_send())

    def settle(k, carry):
        index = (k // zone.plane) * 2 * zone.plane + k % zone.plane
        relay(index, src).wait_send()
        arrived = pltpu.make_async_remote_copy(
            src_ref=src,
            dst_ref=dst_ref.at[index + zone.plane],
            send_sem=send_sem.at[index + zone.plane],
            recv_sem=recv_sem.at[index + zone.plane],
            device_id=zone.partner(),
            device_id_type=MESH,
        )
        arrived.wait_recv()
        return carry

    lax.fori_loop(0, zone.count // 2, settle, 0)


def gathered_force(zone, force_ref, land_ref, send_sem, recv_sem):
    def copy(index):
        return pltpu.make_async_remote_copy(
            src_ref=force_ref.at[index],
            dst_ref=land_ref.at[index],
            send_sem=send_sem.at[index],
            recv_sem=recv_sem.at[index],
            device_id=zone.peer(index, 1),
            device_id_type=MESH,
        )

    if not zone.paired:
        zone.others(lambda index: copy(index).start())
        zone.others(lambda index: copy(index).wait())

        def add(k, total):
            return total + land_ref[(zone.own + 1 + k) % zone.count]

        return lax.fori_loop(0, zone.count - 1, add, force_ref[zone.own])

    def handed(part):
        odd = (2 * part + 1) * zone.plane
        return pltpu.make_async_remote_copy(
            src_ref=force_ref.at[pl.ds(odd, zone.plane)],
            dst_ref=land_ref.at[pl.ds(zone.count + zone.seen_by_partner(odd), zone.plane)],
            send_sem=send_sem.at[odd],
            recv_sem=recv_sem.at[zone.count + zone.seen_by_partner(odd)],
            device_id=zone.partner(),
            device_id_type=MESH,
        )

    def taken(part):
        even = 2 * part * zone.plane
        return pltpu.make_async_remote_copy(
            src_ref=force_ref.at[pl.ds(even, zone.plane)],
            dst_ref=land_ref.at[pl.ds(zone.count + even, zone.plane)],
            send_sem=send_sem.at[even],
            recv_sem=recv_sem.at[zone.count + even],
            device_id=zone.partner(),
            device_id_type=MESH,
        )

    parts = zone.count // (2 * zone.plane)
    for part in range(parts):
        handed(part).start()
    for part in range(parts):
        taken(part).wait_recv()
        even = 2 * part * zone.plane
        for k in range(zone.plane):
            force_ref[even + k] += land_ref[zone.count + even + k]
    zone.alike(lambda index: copy(index).start())
    for part in range(parts):
        handed(part).wait_send()
    zone.alike(lambda index: copy(index).wait())

    def add(k, total):
        return total + land_ref[(k // zone.plane) * 2 * zone.plane + k % zone.plane]

    return lax.fori_loop(1, zone.count // 2, add, force_ref[zone.own])


def weighted(coords, charge):
    charge = 0.125 * charge
    part = jnp.concatenate([charge * c for c in coords] + [charge], axis=0)
    pieces = [p.astype(jnp.float32) for p in split3(part)]
    stacked = jnp.concatenate(pieces + [jnp.zeros_like(part)], axis=0).astype(jnp.bfloat16)
    return jnp.concatenate([stacked, stacked], axis=1)


def folded(out):
    return out[0:4] + out[4:8] + out[8:12]


def shift_of(t):
    t25 = (t * 5243) >> 17
    t5 = (t * 205) >> 10
    return t25 - 2, t5 - 5 * t25 - 2, t - 5 * t5 - 2


def pair_forces(zone, clusters, pairs_ref, x_ref, q_ref, force_ref, left_ref, lw_ref,
                f_ref, right_sum_ref, left_sum_ref, zone_hot_ref, home_hot_ref):
    own = zone.own
    for k in range(clusters):
        coords = []
        for c in range(3):
            row = x_ref[own, pl.ds(c * clusters + k, 1), :]
            coords.append(row)
            left_ref[k, c] = jnp.transpose(jnp.broadcast_to(0.5 * row, (CLUSTER, CLUSTER)))
        lw_ref[k] = weighted(coords, q_ref[own, pl.ds(3 * clusters + k, 1), :])

    def right_side(p):
        j = pairs_ref[1, 0, p]
        deltas = shift_of(pairs_ref[2, 0, p])
        z = zone.place(deltas)
        coords = [
            x_ref[z, pl.ds(c * clusters + j, 1), :] + deltas[c].astype(jnp.float32)
            for c in range(3)
        ]
        return coords, q_ref[z, pl.ds(3 * clusters + j, 1), :]

    def geometry(b):
        for n in range(UNROLL):
            p = b * UNROLL + n
            coords, _ = right_side(p)
            i = pairs_ref[0, 0, p]
            r2 = None
            for c in range(3):
                d = left_ref[i, c] - 0.5 * coords[c]
                r2 = d * d if r2 is None else r2 + d * d
            g = jnp.maximum(1.0 - r2, 0.0)
            den = r2 + 0.125
            start = pl.reciprocal(den, approx=True)
            t = (g * start) * (2.0 - den * start)
            f = (g * t) * (t + 3.0)
            hi = f.astype(jnp.bfloat16)
            f_ref[n, 0] = hi
            f_ref[n, 1] = (f - hi.astype(jnp.float32)).astype(jnp.bfloat16)

    def sums(b):
        found = []
        for n in range(UNROLL):
            p = b * UNROLL + n
            hi, lo = f_ref[n, 0], f_ref[n, 1]
            coords, charge = right_side(p)
            left = lax.dot_general(
                weighted(coords, charge), jnp.concatenate([hi, lo], axis=1),
                (((1,), (1,)), ((), ())), preferred_element_type=jnp.float32,
            )
            right = jnp.dot(
                lw_ref[pairs_ref[0, 0, p]], jnp.concatenate([hi, lo], axis=0),
                preferred_element_type=jnp.float32,
            )
            found.append((p, coords, charge, left, right))
        return found

    def keep(found):
        for p, coords, charge, left, right in found:
            left = folded(left)
            right = folded(right)
            for c in range(4):
                left_sum_ref[c, pl.ds(p, 1), :] = left[c : c + 1]
            for c in range(3):
                right_sum_ref[c, pl.ds(p, 1), :] = charge * (
                    coords[c] * right[3:4] - right[c : c + 1]
                )

    blocks = pairs_ref.shape[2] // UNROLL
    geometry(0)

    def block(b, carry):
        found = sums(b - 1)
        geometry(b)
        keep(found)
        return carry

    lax.fori_loop(1, blocks, block, 0)
    keep(sums(blocks - 1))

    zone_out = exact_dot(zone_hot_ref[...], side_by_side(right_sum_ref))
    home_out = exact_dot(home_hot_ref[...], side_by_side(left_sum_ref))
    for z in range(zone.count):
        for c in range(3):
            force_ref[z, c * clusters : (c + 1) * clusters, :] = zone_out[
                z * 8 : z * 8 + clusters, c * CLUSTER : (c + 1) * CLUSTER
            ]
    for c in range(3):
        rows = slice(c * clusters, (c + 1) * clusters)
        total = home_out[0:clusters, 3 * CLUSTER :]
        moment = home_out[0:clusters, c * CLUSTER : (c + 1) * CLUSTER]
        charge = q_ref[own, 3 * clusters : 4 * clusters, :]
        force_ref[own, rows, :] += charge * (x_ref[own, rows, :] * total - moment)


def kernel(zone, pairs_ref, pairs_vec_ref, x_in, v_in, q_in, atoms_ref, x_out, v_out, f_out,
           zone0_ref, zone1_ref, vel_ref, pos_ref, force_ref, land_ref, slot_ref, left_ref, lw_ref, f_ref,
           right_sum_ref, left_sum_ref, zone_hot_ref, home_hot_ref, send_sem, recv_sem):
    atom_count = x_in.shape[2]
    slots = atoms_ref.shape[1]
    clusters = slots // CLUSTER
    rows = 3 * clusters
    own = zone.own
    barrier = pltpu.get_barrier_semaphore()
    zone.others(lambda index: pl.semaphore_signal(
        barrier, 1, device_id=zone.peer(index, 1), device_id_type=MESH))

    data = jnp.concatenate(
        [x_in[c] for c in range(3)] + [v_in[c] for c in range(3)]
        + [q_in[...], jnp.zeros((1, atom_count), jnp.float32)], axis=0
    )
    hi, mid, lo = split3(data)
    stacked = jnp.concatenate([hi, mid, lo, jnp.zeros_like(hi)], axis=0)
    out = jnp.dot(stacked, one_hot(atoms_ref, atom_count), preferred_element_type=jnp.float32)
    slot = out[0:8] + out[8:16] + out[16:24]
    for k in range(clusters):
        lanes = slice(k * CLUSTER, (k + 1) * CLUSTER)
        for c in range(3):
            zone0_ref[own, c * clusters + k, :] = slot[c, lanes]
            vel_ref[c * clusters + k, :] = slot[3 + c, lanes]
        zone0_ref[own, 3 * clusters + k, :] = slot[6, lanes]
    deltas = shift_of(pairs_vec_ref[2])
    zone_hot_ref[...] = rows_where(zone.count * 8, zone.place(deltas) * 8 + pairs_vec_ref[1])
    home_hot_ref[...] = rows_where(8, pairs_vec_ref[0])
    pl.semaphore_wait(barrier, zone.count - 1)
    share(zone, zone0_ref.at[own], zone0_ref, send_sem.at[0], recv_sem.at[0])

    for step in range(STEPS):
        x_ref = zone0_ref if step == 0 else zone1_ref.at[step - 1]
        pair_forces(zone, clusters, pairs_ref, x_ref, zone0_ref, force_ref, left_ref, lw_ref,
                    f_ref, right_sum_ref, left_sum_ref, zone_hot_ref, home_hot_ref)
        force = gathered_force(zone, force_ref, land_ref.at[step],
                               send_sem.at[2 * step + 1], recv_sem.at[2 * step + 1])
        velocity = vel_ref[...] + TIME_STEP * force
        coords = x_ref[own, 0:rows, :] + TIME_STEP * velocity
        if step < STEPS - 1:
            vel_ref[...] = velocity
            zone1_ref[step, own] = coords
            share(zone, zone1_ref.at[step, own], zone1_ref.at[step],
                  send_sem.at[2 * step + 2], recv_sem.at[2 * step + 2])

    slot_ref[...] = jnp.zeros_like(slot_ref)
    for k in range(clusters):
        lanes = slice(k * CLUSTER, (k + 1) * CLUSTER)
        for c in range(3):
            r = c * clusters + k
            slot_ref[pl.ds(c, 1), lanes] = coords[r : r + 1]
            slot_ref[pl.ds(3 + c, 1), lanes] = velocity[r : r + 1]
            slot_ref[pl.ds(6 + c, 1), lanes] = force[r : r + 1]
    stacked = jnp.concatenate(split3(slot_ref[...]), axis=0)
    out = lax.dot_general(
        stacked, one_hot(atoms_ref, atom_count), (((1,), (1,)), ((), ())),
        preferred_element_type=jnp.float32,
    )
    atom = out[0:16] + out[16:32] + out[32:48]
    for c in range(3):
        x_out[c] = atom[c : c + 1]
        v_out[c] = atom[3 + c : 4 + c]
        f_out[c] = atom[6 + c : 7 + c]


def shards(sizes, positions, velocities, charges, cluster_atoms, pair_list):
    zone = Zone(sizes)
    atom_count = positions.shape[-1]
    slots = cluster_atoms.shape[-1]
    pair_count = pair_list.shape[-1]
    clusters = slots // CLUSTER
    rows = 3 * clusters
    f32, bf16 = jnp.float32, jnp.bfloat16
    x = positions.reshape(3, 1, atom_count)
    v = velocities.reshape(3, 1, atom_count)
    q = charges.reshape(1, atom_count)
    atoms = cluster_atoms.reshape(1, slots)
    pairs = pair_list.reshape(3, 1, pair_count)
    shape = jax.ShapeDtypeStruct((3, 1, atom_count), f32)
    outs = pl.pallas_call(
        functools.partial(kernel, zone),
        out_shape=(shape, shape, shape),
        in_specs=[SMEM] + [VMEM] * 5,
        out_specs=(VMEM, VMEM, VMEM),
        scratch_shapes=[
            pltpu.VMEM((zone.count, 4 * clusters, CLUSTER), f32),
            pltpu.VMEM((STEPS - 1, zone.count, rows, CLUSTER), f32),
            pltpu.VMEM((rows, CLUSTER), f32),
            pltpu.VMEM((rows, CLUSTER), f32),
            pltpu.VMEM((zone.count, rows, CLUSTER), f32),
            pltpu.VMEM((STEPS, 2 * zone.count, rows, CLUSTER), f32),
            pltpu.VMEM((16, slots), f32),
            pltpu.VMEM((clusters, 3, CLUSTER, CLUSTER), f32),
            pltpu.VMEM((clusters, 16, 2 * CLUSTER), bf16),
            pltpu.VMEM((UNROLL, 2, CLUSTER, CLUSTER), bf16),
            pltpu.VMEM((3, pair_count, CLUSTER), f32),
            pltpu.VMEM((4, pair_count, CLUSTER), f32),
            pltpu.VMEM((zone.count * 8, pair_count), bf16),
            pltpu.VMEM((8, pair_count), bf16),
            pltpu.SemaphoreType.DMA((2 * STEPS, 2 * zone.count)),
            pltpu.SemaphoreType.DMA((2 * STEPS, 2 * zone.count)),
        ],
        compiler_params=pltpu.CompilerParams(collective_id=0, has_side_effects=True),
        name="leapfrog",
    )(pairs, pairs, x, v, q, atoms)
    return tuple(out.reshape(positions.shape) for out in outs)


def solution(mesh):
    spec3 = P(None, "gx", "gy", "gz", None)
    spec1 = P("gx", "gy", "gz", None)
    sizes = tuple(mesh.shape[axis] for axis in AXES)
    return jax.shard_map(
        functools.partial(shards, sizes),
        mesh=mesh,
        in_specs=(spec3, spec3, spec1, spec1, spec3),
        out_specs=(spec3, spec3, spec3),
        check_vma=False,
    )
```

```python
import functools

import jax
import jax.numpy as jnp
from jax import lax
from jax.experimental import pallas as pl
from jax.experimental.pallas import tpu as pltpu
from jax.sharding import PartitionSpec as P

CLUSTER = 128
STEPS = 2
TIME_STEP = 0.02
MESH = pl.DeviceIdType.MESH
AXES = ("gx", "gy", "gz")
VMEM = pl.BlockSpec(memory_space=pltpu.VMEM)
SMEM = pl.BlockSpec(memory_space=pltpu.SMEM)
UNROLL = 32


def split3(value):
    hi = value.astype(jnp.bfloat16)
    rest = value - hi.astype(jnp.float32)
    mid = rest.astype(jnp.bfloat16)
    lo = (rest - mid.astype(jnp.float32)).astype(jnp.bfloat16)
    return hi, mid, lo


class Zone:
    def __init__(self, sizes):
        self.sizes = sizes
        self.spans = tuple(min(5, n) for n in sizes)
        self.lows = tuple(-2 if n >= 5 else 0 for n in sizes)
        self.count = self.spans[0] * self.spans[1] * self.spans[2]
        own = tuple(-low for low in self.lows)
        self.paired = max(sizes) <= 4 and sizes[0] % 2 == 0
        self.plane = self.spans[1] * self.spans[2]
        self.own = (own[0] * self.spans[1] + own[1]) * self.spans[2] + own[2]

    def place(self, deltas):
        index = 0
        for delta, n, span in zip(deltas, self.sizes, self.spans):
            if n >= 5:
                here = delta + 2
            elif n in (1, 2, 4):
                here = (delta + 2 * n) & (n - 1)
            else:
                here = lax.rem(delta + 2 * n, n)
            index = index * span + here
        return index

    def peer(self, index, sign):
        parts = (
            index // (self.spans[1] * self.spans[2]),
            (index // self.spans[2]) % self.spans[1],
            index % self.spans[2],
        )
        out = []
        for axis, n, low, part in zip(AXES, self.sizes, self.lows, parts):
            out.append((lax.axis_index(axis) + sign * (part + low) + 2 * n) % n)
        return tuple(out)

    def turn(self):
        return 1 - 2 * (lax.axis_index(AXES[0]) % 2)

    def partner(self):
        return (lax.axis_index(AXES[0]) + self.turn(),) + tuple(
            lax.axis_index(axis) for axis in AXES[1:]
        )

    def seen_by_partner(self, index):
        return (index - self.turn() * self.plane + self.count) % self.count

    def alike(self, body):
        def step(k, carry):
            body((k // self.plane) * 2 * self.plane + k % self.plane)
            return carry

        lax.fori_loop(1, self.count // 2, step, 0)

    def others(self, body):
        def step(k, carry):
            body((self.own + 1 + k) % self.count)
            return carry

        lax.fori_loop(0, self.count - 1, step, 0)


def one_hot(atoms_ref, atom_count):
    slots = atoms_ref.shape[1]
    rows = lax.broadcasted_iota(jnp.int32, (atom_count, slots), 0)
    return jnp.where(rows == atoms_ref[...], 1.0, 0.0).astype(jnp.bfloat16)


def rows_where(count, index):
    rows = lax.broadcasted_iota(jnp.int32, (count, index.shape[1]), 0)
    return jnp.where(rows == index, 1.0, 0.0).astype(jnp.bfloat16)


def exact_dot(selector, values):
    return sum(
        jnp.dot(selector, piece, preferred_element_type=jnp.float32) for piece in split3(values)
    )


def side_by_side(ref):
    return jnp.concatenate([ref[c] for c in range(ref.shape[0])], axis=1)


def share(zone, src, dst_ref, send_sem, recv_sem):
    def copy(index):
        return pltpu.make_async_remote_copy(
            src_ref=src,
            dst_ref=dst_ref.at[index],
            send_sem=send_sem.at[index],
            recv_sem=recv_sem.at[index],
            device_id=zone.peer(index, -1),
            device_id_type=MESH,
        )

    if not zone.paired:
        zone.others(lambda index: copy(index).start())
        zone.others(lambda index: copy(index).wait())
        return

    def relay(index, block):
        place = zone.seen_by_partner(index)
        return pltpu.make_async_remote_copy(
            src_ref=block,
            dst_ref=dst_ref.at[place],
            send_sem=send_sem.at[(index + zone.plane) % zone.count],
            recv_sem=recv_sem.at[place],
            device_id=zone.partner(),
            device_id_type=MESH,
        )

    zone.alike(lambda index: copy(index).start())
    relay(zone.own, src).start()

    def pass_on(index):
        copy(index).wait_recv()
        relay(index, dst_ref.at[index]).start()

    zone.alike(pass_on)
    zone.alike(lambda index: copy(index).wait_send())

    def settle(k, carry):
        index = (k // zone.plane) * 2 * zone.plane + k % zone.plane
        relay(index, src).wait_send()
        arrived = pltpu.make_async_remote_copy(
            src_ref=src,
            dst_ref=dst_ref.at[index + zone.plane],
            send_sem=send_sem.at[index + zone.plane],
            recv_sem=recv_sem.at[index + zone.plane],
            device_id=zone.partner(),
            device_id_type=MESH,
        )
        arrived.wait_recv()
        return carry

    lax.fori_loop(0, zone.count // 2, settle, 0)


def gathered_force(zone, force_ref, land_ref, send_sem, recv_sem):
    def copy(index):
        return pltpu.make_async_remote_copy(
            src_ref=force_ref.at[index],
            dst_ref=land_ref.at[index],
            send_sem=send_sem.at[index],
            recv_sem=recv_sem.at[index],
            device_id=zone.peer(index, 1),
            device_id_type=MESH,
        )

    if not zone.paired:
        zone.others(lambda index: copy(index).start())
        zone.others(lambda index: copy(index).wait())

        def add(k, total):
            return total + land_ref[(zone.own + 1 + k) % zone.count]

        return lax.fori_loop(0, zone.count - 1, add, force_ref[zone.own])

    def handed(part):
        odd = (2 * part + 1) * zone.plane
        return pltpu.make_async_remote_copy(
            src_ref=force_ref.at[pl.ds(odd, zone.plane)],
            dst_ref=land_ref.at[pl.ds(zone.count + zone.seen_by_partner(odd), zone.plane)],
            send_sem=send_sem.at[odd],
            recv_sem=recv_sem.at[zone.count + zone.seen_by_partner(odd)],
            device_id=zone.partner(),
            device_id_type=MESH,
        )

    def taken(part):
        even = 2 * part * zone.plane
        return pltpu.make_async_remote_copy(
            src_ref=force_ref.at[pl.ds(even, zone.plane)],
            dst_ref=land_ref.at[pl.ds(zone.count + even, zone.plane)],
            send_sem=send_sem.at[even],
            recv_sem=recv_sem.at[zone.count + even],
            device_id=zone.partner(),
            device_id_type=MESH,
        )

    parts = zone.count // (2 * zone.plane)
    for part in range(parts):
        handed(part).start()
    for part in range(parts):
        taken(part).wait_recv()
        even = 2 * part * zone.plane
        for k in range(zone.plane):
            force_ref[even + k] += land_ref[zone.count + even + k]
    zone.alike(lambda index: copy(index).start())
    for part in range(parts):
        handed(part).wait_send()
    zone.alike(lambda index: copy(index).wait())

    def add(k, total):
        return total + land_ref[(k // zone.plane) * 2 * zone.plane + k % zone.plane]

    return lax.fori_loop(1, zone.count // 2, add, force_ref[zone.own])


def weighted(coords, charge):
    charge = 0.125 * charge
    part = jnp.concatenate([charge * c for c in coords] + [charge], axis=0)
    pieces = [p.astype(jnp.float32) for p in split3(part)]
    stacked = jnp.concatenate(pieces + [jnp.zeros_like(part)], axis=0).astype(jnp.bfloat16)
    return jnp.concatenate([stacked, stacked], axis=1)


def folded(out):
    return out[0:4] + out[4:8] + out[8:12]


def shift_of(t):
    t25 = (t * 5243) >> 17
    t5 = (t * 205) >> 10
    return t25 - 2, t5 - 5 * t25 - 2, t - 5 * t5 - 2


def pair_forces(zone, clusters, pairs_ref, x_ref, q_ref, force_ref, left_ref, lw_ref,
                f_ref, right_sum_ref, left_sum_ref, zone_hot_ref, home_hot_ref):
    own = zone.own
    for k in range(clusters):
        coords = []
        for c in range(3):
            row = x_ref[own, pl.ds(c * clusters + k, 1), :]
            coords.append(row)
            left_ref[k, c] = jnp.transpose(jnp.broadcast_to(0.5 * row, (CLUSTER, CLUSTER)))
        lw_ref[k] = weighted(coords, q_ref[own, pl.ds(3 * clusters + k, 1), :])

    def right_side(p):
        j = pairs_ref[1, 0, p]
        deltas = shift_of(pairs_ref[2, 0, p])
        z = zone.place(deltas)
        coords = [
            x_ref[z, pl.ds(c * clusters + j, 1), :] + deltas[c].astype(jnp.float32)
            for c in range(3)
        ]
        return coords, q_ref[z, pl.ds(3 * clusters + j, 1), :]

    def geometry(b, which=range(UNROLL)):
        for n in which:
            p = b * UNROLL + n
            coords, _ = right_side(p)
            i = pairs_ref[0, 0, p]
            r2 = None
            for c in range(3):
                d = left_ref[i, c] - 0.5 * coords[c]
                r2 = d * d if r2 is None else r2 + d * d
            g = jnp.maximum(1.0 - r2, 0.0)
            den = r2 + 0.125
            start = pl.reciprocal(den, approx=True)
            t = (g * start) * (2.0 - den * start)
            f = (g * t) * (t + 3.0)
            hi = f.astype(jnp.bfloat16)
            f_ref[n, 0] = hi
            f_ref[n, 1] = (f - hi.astype(jnp.float32)).astype(jnp.bfloat16)

    def sums(b, which=range(UNROLL)):
        found = []
        for n in which:
            p = b * UNROLL + n
            hi, lo = f_ref[n, 0], f_ref[n, 1]
            coords, charge = right_side(p)
            left = lax.dot_general(
                weighted(coords, charge), jnp.concatenate([hi, lo], axis=1),
                (((1,), (1,)), ((), ())), preferred_element_type=jnp.float32,
            )
            right = jnp.dot(
                lw_ref[pairs_ref[0, 0, p]], jnp.concatenate([hi, lo], axis=0),
                preferred_element_type=jnp.float32,
            )
            found.append((p, coords, charge, left, right))
        return found

    def keep(found):
        for p, coords, charge, left, right in found:
            left = folded(left)
            right = folded(right)
            for c in range(4):
                left_sum_ref[c, pl.ds(p, 1), :] = left[c : c + 1]
            for c in range(3):
                right_sum_ref[c, pl.ds(p, 1), :] = charge * (
                    coords[c] * right[3:4] - right[c : c + 1]
                )

    blocks = pairs_ref.shape[2] // UNROLL
    geometry(0)

    def block(b, carry):
        found = []
        for n in range(UNROLL):
            found += sums(b - 1, [n])
            geometry(b, [n])
            if n > 1:
                keep(found[n - 2 : n - 1])
        keep(found[-2:])
        return carry

    lax.fori_loop(1, blocks, block, 0)
    keep(sums(blocks - 1))

    zone_out = exact_dot(zone_hot_ref[...], side_by_side(right_sum_ref))
    home_out = exact_dot(home_hot_ref[...], side_by_side(left_sum_ref))
    for z in range(zone.count):
        for c in range(3):
            force_ref[z, c * clusters : (c + 1) * clusters, :] = zone_out[
                z * 8 : z * 8 + clusters, c * CLUSTER : (c + 1) * CLUSTER
            ]
    for c in range(3):
        rows = slice(c * clusters, (c + 1) * clusters)
        total = home_out[0:clusters, 3 * CLUSTER :]
        moment = home_out[0:clusters, c * CLUSTER : (c + 1) * CLUSTER]
        charge = q_ref[own, 3 * clusters : 4 * clusters, :]
        force_ref[own, rows, :] += charge * (x_ref[own, rows, :] * total - moment)


def kernel(zone, pairs_ref, pairs_vec_ref, x_in, v_in, q_in, atoms_ref, x_out, v_out, f_out,
           zone0_ref, zone1_ref, vel_ref, pos_ref, force_ref, land_ref, slot_ref, left_ref, lw_ref, f_ref,
           right_sum_ref, left_sum_ref, zone_hot_ref, home_hot_ref, send_sem, recv_sem):
    atom_count = x_in.shape[2]
    slots = atoms_ref.shape[1]
    clusters = slots // CLUSTER
    rows = 3 * clusters
    own = zone.own
    barrier = pltpu.get_barrier_semaphore()
    zone.others(lambda index: pl.semaphore_signal(
        barrier, 1, device_id=zone.peer(index, 1), device_id_type=MESH))

    data = jnp.concatenate(
        [x_in[c] for c in range(3)] + [v_in[c] for c in range(3)]
        + [q_in[...], jnp.zeros((1, atom_count), jnp.float32)], axis=0
    )
    hi, mid, lo = split3(data)
    stacked = jnp.concatenate([hi, mid, lo, jnp.zeros_like(hi)], axis=0)
    out = jnp.dot(stacked, one_hot(atoms_ref, atom_count), preferred_element_type=jnp.float32)
    slot = out[0:8] + out[8:16] + out[16:24]
    for k in range(clusters):
        lanes = slice(k * CLUSTER, (k + 1) * CLUSTER)
        for c in range(3):
            zone0_ref[own, c * clusters + k, :] = slot[c, lanes]
            vel_ref[c * clusters + k, :] = slot[3 + c, lanes]
        zone0_ref[own, 3 * clusters + k, :] = slot[6, lanes]
    deltas = shift_of(pairs_vec_ref[2])
    zone_hot_ref[...] = rows_where(zone.count * 8, zone.place(deltas) * 8 + pairs_vec_ref[1])
    home_hot_ref[...] = rows_where(8, pairs_vec_ref[0])
    pl.semaphore_wait(barrier, zone.count - 1)
    share(zone, zone0_ref.at[own], zone0_ref, send_sem.at[0], recv_sem.at[0])

    for step in range(STEPS):
        x_ref = zone0_ref if step == 0 else zone1_ref.at[step - 1]
        pair_forces(zone, clusters, pairs_ref, x_ref, zone0_ref, force_ref, left_ref, lw_ref,
                    f_ref, right_sum_ref, left_sum_ref, zone_hot_ref, home_hot_ref)
        force = gathered_force(zone, force_ref, land_ref.at[step],
                               send_sem.at[2 * step + 1], recv_sem.at[2 * step + 1])
        velocity = vel_ref[...] + TIME_STEP * force
        coords = x_ref[own, 0:rows, :] + TIME_STEP * velocity
        if step < STEPS - 1:
            vel_ref[...] = velocity
            zone1_ref[step, own] = coords
            share(zone, zone1_ref.at[step, own], zone1_ref.at[step],
                  send_sem.at[2 * step + 2], recv_sem.at[2 * step + 2])

    slot_ref[...] = jnp.zeros_like(slot_ref)
    for k in range(clusters):
        lanes = slice(k * CLUSTER, (k + 1) * CLUSTER)
        for c in range(3):
            r = c * clusters + k
            slot_ref[pl.ds(c, 1), lanes] = coords[r : r + 1]
            slot_ref[pl.ds(3 + c, 1), lanes] = velocity[r : r + 1]
            slot_ref[pl.ds(6 + c, 1), lanes] = force[r : r + 1]
    stacked = jnp.concatenate(split3(slot_ref[...]), axis=0)
    out = lax.dot_general(
        stacked, one_hot(atoms_ref, atom_count), (((1,), (1,)), ((), ())),
        preferred_element_type=jnp.float32,
    )
    atom = out[0:16] + out[16:32] + out[32:48]
    for c in range(3):
        x_out[c] = atom[c : c + 1]
        v_out[c] = atom[3 + c : 4 + c]
        f_out[c] = atom[6 + c : 7 + c]


def shards(sizes, positions, velocities, charges, cluster_atoms, pair_list):
    zone = Zone(sizes)
    atom_count = positions.shape[-1]
    slots = cluster_atoms.shape[-1]
    pair_count = pair_list.shape[-1]
    clusters = slots // CLUSTER
    rows = 3 * clusters
    f32, bf16 = jnp.float32, jnp.bfloat16
    x = positions.reshape(3, 1, atom_count)
    v = velocities.reshape(3, 1, atom_count)
    q = charges.reshape(1, atom_count)
    atoms = cluster_atoms.reshape(1, slots)
    pairs = pair_list.reshape(3, 1, pair_count)
    shape = jax.ShapeDtypeStruct((3, 1, atom_count), f32)
    outs = pl.pallas_call(
        functools.partial(kernel, zone),
        out_shape=(shape, shape, shape),
        in_specs=[SMEM] + [VMEM] * 5,
        out_specs=(VMEM, VMEM, VMEM),
        scratch_shapes=[
            pltpu.VMEM((zone.count, 4 * clusters, CLUSTER), f32),
            pltpu.VMEM((STEPS - 1, zone.count, rows, CLUSTER), f32),
            pltpu.VMEM((rows, CLUSTER), f32),
            pltpu.VMEM((rows, CLUSTER), f32),
            pltpu.VMEM((zone.count, rows, CLUSTER), f32),
            pltpu.VMEM((STEPS, 2 * zone.count, rows, CLUSTER), f32),
            pltpu.VMEM((16, slots), f32),
            pltpu.VMEM((clusters, 3, CLUSTER, CLUSTER), f32),
            pltpu.VMEM((clusters, 16, 2 * CLUSTER), bf16),
            pltpu.VMEM((UNROLL, 2, CLUSTER, CLUSTER), bf16),
            pltpu.VMEM((3, pair_count, CLUSTER), f32),
            pltpu.VMEM((4, pair_count, CLUSTER), f32),
            pltpu.VMEM((zone.count * 8, pair_count), bf16),
            pltpu.VMEM((8, pair_count), bf16),
            pltpu.SemaphoreType.DMA((2 * STEPS, 2 * zone.count)),
            pltpu.SemaphoreType.DMA((2 * STEPS, 2 * zone.count)),
        ],
        compiler_params=pltpu.CompilerParams(collective_id=0, has_side_effects=True),
        name="leapfrog",
    )(pairs, pairs, x, v, q, atoms)
    return tuple(out.reshape(positions.shape) for out in outs)


def solution(mesh):
    spec3 = P(None, "gx", "gy", "gz", None)
    spec1 = P("gx", "gy", "gz", None)
    sizes = tuple(mesh.shape[axis] for axis in AXES)
    return jax.shard_map(
        functools.partial(shards, sizes),
        mesh=mesh,
        in_specs=(spec3, spec3, spec1, spec1, spec3),
        out_specs=(spec3, spec3, spec3),
        check_vma=False,
    )
```
